256 devices in a mesh: front: 16 (over z, core), row: 4 (over y), col: 4 (over x).
Axes of the slice: x: 4, y: 4, z: 8, core: 2. Of those that a mesh axis runs over, the one named last changes fastest.
Arguments:
- child_blocks: bfloat16 [131072, 8192], P(('front', 'row'), 'col'), may hold values from -0.0625 to 0.0625
- sketch: bfloat16 [8192, 512], P('col'), may hold values from -6 to 6
- block_map: int32 [16, 64], P('front'), may hold values from 0 to 95, as said below
Outputs:
- parent_basis: float32 [512, 49152], P('col', ('front', 'row'))
The draws below stay inside these ranges and needn't reach their ends.
Inputs may be any that keep to these rules, and one draw needn't show every extreme that they name: `block_map`: each row lists 8192 / 128 different parent blocks in increasing order.
All inputs are finite; a program needn't handle non-finite values.
Results may differ from the reference program's by a relative error of at most 0.0003.
Values sent between devices are 32-bit elements; how exact they have to be, the bound alone decides.
A program may use at most 128 MiB of HBM per device.

```python
import jax
import jax.numpy as jnp
from jax import lax

F = 8192
P_SIZE = 12288
S = 512
BLK = 128
R = 8192
CHILDREN = 16
SIBS = 4
PARENTS = 4


def draw_block_map(key, part):
    child_keys = jax.random.split(jax.random.fold_in(key, 7), CHILDREN)

    def one_child(child_key):
        chosen = jax.random.permutation(child_key, P_SIZE // BLK)[:R // BLK]
        return jnp.sort(chosen)
    return jax.vmap(one_child)(child_keys).astype(jnp.int32)


def shard_levels(stream_key, extent, shards, low, high):
    factor_of, own = 1.0, jax.random.fold_in(stream_key, 6)
    for axis_at, parts in shards:
        draws = jnp.exp(jax.random.uniform(jax.random.fold_in(own, axis_at), (parts,), jnp.float32, low / len(shards), high / len(shards)))
        factor_of = factor_of * jnp.repeat(draws, extent[axis_at] // parts).reshape([-1 if axis == axis_at else 1 for axis in range(len(extent))])
    return factor_of


def scatter_about(key, shape, width, bound, cuts=(), held_as=jnp.bfloat16):
    factor_of = shard_levels(key, shape, cuts, -0.22, 0.18) if cuts else 1.0
    drawn = jax.random.normal(key, shape, jnp.float32) * width * factor_of
    return jnp.minimum(jnp.maximum(drawn, -bound), bound).astype(held_as)


def setup_inputs(seed: int = 0) -> dict:
    seeds = jax.random.split(jax.random.key(seed), 4)
    return {
        "child_blocks": scatter_about(seeds[0], (CHILDREN * R, F), F ** -0.5, 0.0625, ((0, 64), (1, 4))),
        "sketch": scatter_about(seeds[1], (F, S), 1.0, 6.0, ((0, 4),)),
        "block_map": draw_block_map(jax.random.fold_in(seeds[3], 71), 0),
    }


def reference(child_blocks, sketch, block_map):
    panels = child_blocks.reshape(CHILDREN, R, F)

    def child_product(panel):
        return jnp.dot(panel.astype(jnp.float32), sketch.astype(jnp.float32), preferred_element_type=jnp.float32)
    sketch_rows = lax.map(child_product, panels)
    targets = jnp.arange(P_SIZE // BLK, dtype=jnp.int32)
    results = []
    for parent in range(PARENTS):
        extended = jnp.zeros((P_SIZE // BLK, BLK, S), jnp.float32)
        for sibling in range(SIBS):
            child = parent * SIBS + sibling
            one_hot = (block_map[child][:, None] == targets[None, :]).astype(jnp.float32)
            blocks = sketch_rows[child].reshape(R // BLK, BLK, S)
            extended = extended + jnp.einsum('bm,bks->mks', one_hot, blocks, precision=lax.Precision.HIGHEST)
        parent_sketch = extended.reshape(P_SIZE, S)
        gram = jnp.dot(parent_sketch.T, parent_sketch, precision=lax.Precision.HIGHEST)
        lower = jnp.linalg.cholesky(gram)
        results.append(jax.scipy.linalg.solve_triangular(lower, parent_sketch.T, lower=True))
    return jnp.concatenate(results, axis=1)
```

```python
import jax
import jax.numpy as jnp
from jax import lax
from jax.experimental import pallas as pl
from jax.experimental.pallas import tpu as pltpu
from jax.sharding import PartitionSpec as P

MESH = pl.DeviceIdType.MESH
HIGHEST = lax.Precision.HIGHEST
VMEM = pl.BlockSpec(memory_space=pltpu.VMEM)
BLK = 128
PARENT_BLOCKS = 96
SUB = 32
SRC = 16
OWN = 6
STAGES = [(q, g) for q in range(4) for g in range(2)]
SLICE_OF_STEP = ((0, 2, 1), (1, 2, 0))


def remote(src, dst, send, recv, **where):
    return pltpu.make_async_remote_copy(
        src_ref=src, dst_ref=dst, send_sem=send, recv_sem=recv, device_id=where, device_id_type=MESH
    )


def meet(peers):
    barrier = pltpu.get_barrier_semaphore()
    for where in peers:
        pl.semaphore_signal(barrier, inc=1, device_id=where, device_id_type=MESH)
    pl.semaphore_wait(barrier, len(peers))


def around(axis):
    here = lax.axis_index(axis)
    return here, [lax.rem(here + step, 4) for step in range(4)]


def flip(front, bits):
    low = lax.rem(front, 4)
    core, half = lax.rem(low, 2), low // 2
    if bits & 1:
        core = 1 - core
    if bits & 2:
        half = 1 - half
    return front - low + 2 * half + core


def share_kernel(
    a_hbm, om_hbm, map_ref, s_ref,
    a_v, om_v, part, xr, ys, yr, tab_v, tab_s,
    a_sem, om_sem, tab_sem, tab_ss, tab_rs, x_ss, x_rs, c_ss, c_rs, z_ss, z_rs, f_ss, f_rs, y_ss, y_rs,
    *gats,
):
    front = lax.axis_index("front")
    sibling = lax.rem(front, 4)
    row, rows = around("row")
    col, cols = around("col")
    near = [flip(front, bits) for bits in range(4)]
    pending = []

    om_copy = pltpu.make_async_copy(om_hbm, om_v, om_sem)
    om_copy.start()
    a_copies = []
    for i, s in enumerate((cols[3], cols[1], cols[2], col)):
        copy = pltpu.make_async_copy(
            a_hbm.at[:, pl.ds(pl.multiple_of(s * SUB, SUB), SUB), :], a_v.at[i], a_sem.at[i]
        )
        copy.start()
        a_copies.append(copy)

    meet(
        [{"col": cols[1]}, {"col": cols[3]}]
        + [{"row": rows[k]} for k in (1, 2, 3)]
        + [{"front": near[k]} for k in (1, 2, 3)]
    )

    lane = lax.broadcasted_iota(jnp.int32, (8, BLK), 1)
    table = jnp.full((8, BLK), SRC, jnp.int32)
    for b in range(SRC):
        table = jnp.where(lane == map_ref[0, row * SRC + b], b, table)
    tab_v[0] = table
    tab_copies = []
    for k in (1, 2, 3):
        copy = remote(tab_v.at[0], tab_v.at[k], tab_ss.at[k - 1], tab_rs.at[k - 1], front=near[k])
        copy.start()
        tab_copies.append(copy)
    for gat in gats:
        for k in range(4):
            gat[k, SRC] = jnp.zeros((8, BLK), jnp.float32)

    def multiply(i, h):
        part[i, :, :, 256 * h : 256 * h + 256] = jnp.dot(
            a_v[i].reshape(SRC * SUB, a_v.shape[-1]),
            om_v[:, 256 * h : 256 * h + 256],
            preferred_element_type=jnp.float32,
        ).reshape(SRC, SUB, 256)

    def piece(t, d, i):
        q, g = STAGES[t]
        lo = 256 * d + BLK * g
        return (i, slice(None), slice(8 * q, 8 * q + 8), slice(lo, lo + BLK))

    x_copy, c_copy, z_copy, f_copy, y_copy = {}, {}, {}, {}, {}

    def send_x(t, d, step):
        copy = remote(
            part.at[piece(t, d, SLICE_OF_STEP[d][step])], xr.at[t, d, step],
            x_ss.at[t, d, step], x_rs.at[t, d, step], col=cols[1] if d == 0 else cols[3],
        )
        copy.start()
        x_copy[t, d, step] = copy
        pending.append(copy)

    def pass_x(t, d, step):
        x_copy[t, d, step - 1].wait_recv()
        at = piece(t, d, SLICE_OF_STEP[d][step])
        part[at] = part[at] + xr[t, d, step - 1]
        send_x(t, d, step)

    def finish_x(t, d):
        x_copy[t, d, 2].wait_recv()
        gat = gats[2 * t + d]
        gat[0, :SRC] = part[piece(t, d, 3)] + xr[t, d, 2]
        z = remote(gat.at[0, :SRC], gat.at[2, :SRC], z_ss.at[t, d], z_rs.at[t, d], front=near[2])
        z.start()
        c = remote(gat.at[0, :SRC], gat.at[1, :SRC], c_ss.at[t, d], c_rs.at[t, d], front=near[1])
        c.start()
        z_copy[t, d], c_copy[t, d] = z, c
        pending.extend((z, c))

    def forward_z(t, d):
        z_copy[t, d].wait_recv()
        gat = gats[2 * t + d]
        copy = remote(gat.at[2, :SRC], gat.at[3, :SRC], f_ss.at[t, d], f_rs.at[t, d], front=near[1])
        copy.start()
        f_copy[t, d] = copy
        pending.append(copy)

    def merge(t, d):
        c_copy[t, d].wait_recv()
        f_copy[t, d].wait_recv()
        gat = gats[2 * t + d]
        for j in range(4 * OWN):
            at = sibling * (4 * OWN) + j
            ys[t, d, j] = (gat[0, tab_s[0, 0, at]] + gat[1, tab_s[1, 0, at]]) + (
                gat[2, tab_s[2, 0, at]] + gat[3, tab_s[3, 0, at]]
            )
        for k in (1, 2, 3):
            copy = remote(
                ys.at[t, d, pl.ds(OWN * rows[k], OWN)], yr.at[t, d, k - 1],
                y_ss.at[t, d, k - 1], y_rs.at[t, d, k - 1], row=rows[k],
            )
            copy.start()
            y_copy[t, d, k] = copy
            pending.append(copy)

    def finish_y(t, d):
        for k in (1, 2, 3):
            y_copy[t, d, k].wait_recv()
        _, _, at_rows, at_cols = piece(t, d, 0)
        s_ref[:, at_rows, at_cols] = (ys[t, d, pl.ds(OWN * row, OWN)] + yr[t, d, 0]) + (
            yr[t, d, 1] + yr[t, d, 2]
        )

    om_copy.wait()
    a_copies[0].wait()
    multiply(0, 0)
    send_x(0, 0, 0)
    send_x(1, 0, 0)
    a_copies[1].wait()
    multiply(1, 1)
    send_x(0, 1, 0)
    send_x(1, 1, 0)
    send_x(2, 0, 0)
    send_x(2, 1, 0)
    a_copies[2].wait()
    a_copies[3].wait()
    for i, h in ((2, 0), (2, 1), (1, 0), (0, 1), (3, 0), (3, 1)):
        multiply(i, h)
    for copy in tab_copies:
        copy.wait()
    tab_copy = pltpu.make_async_copy(tab_v, tab_s, tab_sem)
    tab_copy.start()
    tab_copy.wait()

    count = len(STAGES)
    for tick in range(1, count + 6):
        for action, lag in (
            (lambda t, d: pass_x(t, d, 1), 1),
            (lambda t, d: pass_x(t, d, 2), 2),
            (finish_x, 3),
            (lambda t, d: send_x(t, d, 0), -2),
            (forward_z, 4),
            (merge, 5),
            (finish_y, 6),
        ):
            t = tick - lag
            if t in range(count) and not (lag == -2 and t < 3):
                for d in (0, 1):
                    action(t, d)
    for copy in pending:
        copy.wait_send()


def gram_kernel(
    s_ref, g_ref, all_ref,
    mine, r1, a1, r2, a2, r3, a3, r4,
    c_ss, c_rs, y_ss, y_rs, z_ss, z_rs, x_ss, x_rs, b_ss, b_rs, e_ss, e_rs, s_ss, s_rs, w_ss, w_rs,
):
    front = lax.axis_index("front")
    core = lax.rem(front, 2)
    row, rows = around("row")
    col, cols = around("col")
    near = [flip(front, bits) for bits in range(4)]
    half = 5 * BLK
    fourth = half // 4
    meet(
        [{"col": cols[k]} for k in (1, 2, 3)]
        + [{"row": rows[k]} for k in (1, 2, 3)]
        + [{"front": near[k]} for k in (1, 2)]
    )
    shared = []
    for d in (0, 1):
        copy = remote(s_ref, all_ref.at[:, col], s_ss.at[d], s_rs.at[d], col=cols[1] if d == 0 else cols[3])
        copy.start()
        shared.append(copy)
    all_ref[:, col] = s_ref[...]

    s = s_ref[...].reshape(OWN * SUB, 4 * BLK)
    at = 0
    for i in range(4):
        panel = lax.dot_general(
            s[:, BLK * i : BLK * i + BLK], s[:, BLK * i :], (((0,), (0,)), ((), ())),
            precision=HIGHEST, preferred_element_type=jnp.float32,
        )
        for k in range(4 - i):
            mine[at : at + BLK] = panel[:, BLK * k : BLK * k + BLK]
            at += BLK
    keep = pl.ds(pl.multiple_of(half * core, BLK), half)
    give = pl.ds(pl.multiple_of(half * (1 - core), BLK), half)
    c_copy = remote(mine.at[give], r1, c_ss, c_rs, front=near[1])
    c_copy.start()
    c_copy.wait_recv()
    a1[...] = mine[keep] + r1[...]
    y_copies = []
    for k in (1, 2, 3):
        copy = remote(
            a1.at[pl.ds(pl.multiple_of(fourth * rows[k], 8), fourth)], r2.at[k - 1],
            y_ss.at[k - 1], y_rs.at[k - 1], row=rows[k],
        )
        copy.start()
        y_copies.append(copy)
    for copy in y_copies:
        copy.wait_recv()
    a2[...] = (a1[pl.ds(pl.multiple_of(fourth * row, 8), fourth)] + r2[0]) + (r2[1] + r2[2])
    z_copy = remote(a2, r3, z_ss, z_rs, front=near[2])
    z_copy.start()
    for copy in shared:
        copy.wait_recv()
    passed = []
    for d in (0, 1):
        block = all_ref.at[:, cols[3] if d == 0 else cols[1], 16 * d : 16 * d + 16]
        copy = remote(block, block, w_ss.at[d], w_rs.at[d], col=cols[1] if d == 0 else cols[3])
        copy.start()
        passed.append(copy)
    z_copy.wait_recv()
    a3[...] = a2[...] + r3[...]
    x_copies = []
    for k in (1, 2, 3):
        copy = remote(a3, r4.at[k - 1], x_ss.at[k - 1], x_rs.at[k - 1], col=cols[k])
        copy.start()
        x_copies.append(copy)
    for copy in x_copies:
        copy.wait_recv()
    mid = pl.ds(pl.multiple_of(half * core + fourth * row, 8), fourth)
    g_ref[mid] = (a3[...] + r4[0]) + (r4[1] + r4[2])
    b_copies = []
    for k in (1, 2, 3):
        copy = remote(g_ref.at[mid], g_ref.at[mid], b_ss.at[k - 1], b_rs.at[k - 1], row=rows[k])
        copy.start()
        b_copies.append(copy)
    for copy in b_copies:
        copy.wait_recv()
    e_copy = remote(g_ref.at[keep], g_ref.at[keep], e_ss, e_rs, front=near[1])
    e_copy.start()
    e_copy.wait_recv()
    for copy in passed:
        copy.wait_recv()
    for copy in [c_copy, *y_copies, z_copy, *x_copies, *b_copies, e_copy, *shared, *passed]:
        copy.wait_send()


def factor_inverse(read, write):
    sub = lax.broadcasted_iota(jnp.int32, (8, BLK), 0)
    lane = lax.broadcasted_iota(jnp.int32, (8, BLK), 1)
    count = BLK // 8
    upper = [read(i) for i in range(count)]
    inverse = [jnp.where(lane == sub + 8 * i, 1.0, 0.0).astype(jnp.float32) for i in range(count)]

    def spread(block, k):
        return jnp.broadcast_to(block[k : k + 1, :], (8, BLK))

    for j in range(count):
        below = range(j, count)
        column = {
            i: [jnp.broadcast_to(upper[i][:, 8 * j + k : 8 * j + k + 1], (8, BLK)) for k in range(8)]
            for i in below
        }
        lower = {i: [] for i in below}
        rest, solved = upper[j], inverse[j]
        u_rows, w_rows = [], []
        for k in range(8):
            scale = lax.rsqrt(spread(column[j][k], k))
            for i in below:
                lower[i].append(column[i][k] * scale)
            u_row, w_row = spread(rest, k) * scale, spread(solved, k) * scale
            u_rows.append(u_row)
            w_rows.append(w_row)
            under = jnp.where(sub > k, lower[j][k], 0.0)
            solved = jnp.where(sub == k, w_row, solved - under * w_row)
            rest = rest - under * u_row
            for later in range(k + 1, 8):
                factor = spread(lower[j][k], later)
                for i in below:
                    column[i][later] = column[i][later] - lower[i][k] * factor
        write(j, solved)
        for i in range(j + 1, count):
            for k in range(8):
                upper[i] = upper[i] - lower[i][k] * u_rows[k]
                inverse[i] = inverse[i] - lower[i][k] * w_rows[k]


def basis_kernel(g_ref, all_ref, out_ref, a, v):
    def dot(x, y, dims):
        return lax.dot_general(x, y, (dims, ((), ())), precision=HIGHEST, preferred_element_type=jnp.float32)

    at = 0
    for i in range(4):
        for k in range(i, 4):
            a[i, :, BLK * k : BLK * k + BLK] = g_ref[at : at + BLK]
            at += BLK
    v[...] = jnp.zeros_like(v)
    for j in range(4):
        here = slice(BLK * j, BLK * j + BLK)

        def read(i):
            return a[j, 8 * i : 8 * i + 8, here]

        def write(i, rows):
            v[j, 8 * i : 8 * i + 8, here] = rows

        factor_inverse(read, write)
        w = v[j, :, here]
        if j:
            v[j, :, : BLK * j] = dot(w, v[j, :, : BLK * j], ((1,), (0,)))
        if j < 3:
            u = dot(w, a[j, :, BLK * (j + 1) :], ((1,), (0,)))
            for i in range(j + 1, 4):
                left = u[:, BLK * (i - j - 1) : BLK * (i - j)]
                a[i, :, BLK * i :] = a[i, :, BLK * i :] - dot(left, u[:, BLK * (i - j - 1) :], ((0,), (0,)))
                v[i, :, : BLK * (j + 1)] = v[i, :, : BLK * (j + 1)] - dot(
                    left, v[j, :, : BLK * (j + 1)], ((0,), (0,))
                )
    mine = v[lax.axis_index("col")]
    out_ref[...] = dot(mine, all_ref[...].reshape(OWN * BLK, 4 * BLK), ((1,), (1,)))


def shards(child_blocks, sketch, block_map):
    f32, dma = jnp.float32, pltpu.SemaphoreType.DMA
    stages = len(STAGES)
    depth, width = sketch.shape
    share = pl.pallas_call(
        share_kernel,
        out_shape=jax.ShapeDtypeStruct((OWN, SUB, width), f32),
        in_specs=[
            pl.BlockSpec(memory_space=pl.ANY),
            pl.BlockSpec(memory_space=pl.ANY),
            pl.BlockSpec(memory_space=pltpu.SMEM),
        ],
        out_specs=VMEM,
        scratch_shapes=[
            pltpu.VMEM((4, SRC, SUB, depth), jnp.bfloat16),
            pltpu.VMEM((depth, width), jnp.bfloat16),
            pltpu.VMEM((4, SRC, SUB, width), f32),
            pltpu.VMEM((stages, 2, 3, SRC, 8, BLK), f32),
            pltpu.VMEM((stages, 2, 4 * OWN, 8, BLK), f32),
            pltpu.VMEM((stages, 2, 3, OWN, 8, BLK), f32),
            pltpu.VMEM((4, 8, BLK), jnp.int32),
            pltpu.SMEM((4, 8, BLK), jnp.int32),
            dma((4,)), dma, dma, dma((3,)), dma((3,)),
            dma((stages, 2, 3)), dma((stages, 2, 3)),
            dma((stages, 2)), dma((stages, 2)),
            dma((stages, 2)), dma((stages, 2)),
            dma((stages, 2)), dma((stages, 2)),
            dma((stages, 2, 3)), dma((stages, 2, 3)),
        ]
        + [pltpu.VMEM((4, SRC + 1, 8, BLK), f32)] * (2 * stages),
        compiler_params=pltpu.CompilerParams(collective_id=0, has_side_effects=True, vmem_limit_bytes=48 << 20),
        name="share",
    )(child_blocks.reshape(SRC, BLK, depth), sketch, block_map)
    gram, everyone = pl.pallas_call(
        gram_kernel,
        out_shape=(
            jax.ShapeDtypeStruct((10 * BLK, BLK), f32),
            jax.ShapeDtypeStruct((OWN, 4, SUB, width), f32),
        ),
        in_specs=[VMEM],
        out_specs=(VMEM, VMEM),
        scratch_shapes=[
            pltpu.VMEM((10 * BLK, BLK), f32),
            pltpu.VMEM((5 * BLK, BLK), f32),
            pltpu.VMEM((5 * BLK, BLK), f32),
            pltpu.VMEM((3, 5 * BLK // 4, BLK), f32),
            pltpu.VMEM((5 * BLK // 4, BLK), f32),
            pltpu.VMEM((5 * BLK // 4, BLK), f32),
            pltpu.VMEM((5 * BLK // 4, BLK), f32),
            pltpu.VMEM((3, 5 * BLK // 4, BLK), f32),
            dma, dma, dma((3,)), dma((3,)), dma, dma, dma((3,)), dma((3,)),
            dma((3,)), dma((3,)), dma, dma, dma((2,)), dma((2,)), dma((2,)), dma((2,)),
        ],
        compiler_params=pltpu.CompilerParams(collective_id=1, has_side_effects=True),
        name="gram",
    )(share)
    return pl.pallas_call(
        basis_kernel,
        out_shape=jax.ShapeDtypeStruct((BLK, OWN * BLK), f32),
        in_specs=[VMEM, VMEM],
        out_specs=VMEM,
        scratch_shapes=[pltpu.VMEM((4, BLK, 4 * BLK), f32), pltpu.VMEM((4, BLK, 4 * BLK), f32)],
        name="basis",
    )(gram, everyone)


def solution(mesh):
    placed = (P(("front", "row"), "col"), P("col", None), P("front", None))
    return jax.shard_map(
        shards, mesh=mesh, in_specs=placed, out_specs=P("col", ("front", "row")), check_vma=False
    )
```

```python
import jax
import jax.numpy as jnp
from jax import lax
from jax.experimental import pallas as pl
from jax.experimental.pallas import tpu as pltpu
from jax.sharding import PartitionSpec as P

MESH = pl.DeviceIdType.MESH
HIGHEST = lax.Precision.HIGHEST
BLK = 128
SUB = 32
SRC = 16
OWN = 6
HALF = 256
STAGES = [(0, 0, 256), (1, 0, 256), (2, 0, 256), (3, 0, 128), (3, 128, 128)]
PARTS = ((0, 4 * BLK), (4 * BLK, 6 * BLK))


def remote(src, dst, send, recv, **where):
    copy = pltpu.make_async_remote_copy(
        src_ref=src, dst_ref=dst, send_sem=send, recv_sem=recv, device_id=where, device_id_type=MESH
    )
    copy.start()
    return copy


def around(axis):
    here = lax.axis_index(axis)
    return here, [lax.rem(here + step, 4) for step in range(4)]


def flip(front, bits):
    low = lax.rem(front, 4)
    core, half = lax.rem(low, 2), low // 2
    if bits & 1:
        core = 1 - core
    if bits & 2:
        half = 1 - half
    return front - low + 2 * half + core


def dot(x, y, dims):
    return lax.dot_general(x, y, (dims, ((), ())), precision=HIGHEST, preferred_element_type=jnp.float32)


def factor_inverse(read, write):
    sub = lax.broadcasted_iota(jnp.int32, (8, BLK), 0)
    lane = lax.broadcasted_iota(jnp.int32, (8, BLK), 1)
    count = BLK // 8
    upper = [read(i) for i in range(count)]
    inverse = [jnp.where(lane == sub + 8 * i, 1.0, 0.0).astype(jnp.float32) for i in range(count)]

    def spread(block, k):
        return jnp.broadcast_to(block[k : k + 1, :], (8, BLK))

    for j in range(count):
        below = range(j, count)
        column = {
            i: [jnp.broadcast_to(upper[i][:, 8 * j + k : 8 * j + k + 1], (8, BLK)) for k in range(8)]
            for i in below
        }
        lower = {i: [] for i in below}
        rest, solved = upper[j], inverse[j]
        u_rows, w_rows = [], []
        for k in range(8):
            scale = lax.rsqrt(spread(column[j][k], k))
            for i in below:
                lower[i].append(column[i][k] * scale)
            u_row, w_row = spread(rest, k) * scale, spread(solved, k) * scale
            u_rows.append(u_row)
            w_rows.append(w_row)
            under = jnp.where(sub > k, lower[j][k], 0.0)
            solved = jnp.where(sub == k, w_row, solved - under * w_row)
            rest = rest - under * u_row
            for later in range(k + 1, 8):
                factor = spread(lower[j][k], later)
                for i in below:
                    column[i][later] = column[i][later] - lower[i][k] * factor
        write(j, solved)
        for i in range(j + 1, count):
            for k in range(8):
                upper[i] = upper[i] - lower[i][k] * u_rows[k]
                inverse[i] = inverse[i] - lower[i][k] * w_rows[k]


def kernel(a_hbm, om_hbm, map_ref, out_ref, *scratch):
    left = iter(scratch)

    def take(count):
        return [next(left) for _ in range(count)]

    a_v, om_v, part, tab_v, tab_s, all_v, mine, gram, a, v = take(10)
    a_sem, om_sem, tab_sem, tab_ss, tab_rs = take(5)
    x_ss, x_rs, c_ss, c_rs, z_ss, z_rs, f_ss, f_rs, y_ss, y_rs, s_ss, s_rs, w_ss, w_rs = take(14)
    stage_refs = [take(5) for _ in STAGES]
    part_refs = [take(14) for _ in PARTS]

    front = lax.axis_index("front")
    sibling, core = lax.rem(front, 4), lax.rem(front, 2)
    row, rows = around("row")
    col, cols = around("col")
    near = [flip(front, bits) for bits in range(4)]
    spots = [(i, j) for i in range(4) for j in range(4)]
    pending = []

    def note(copy):
        pending.append(copy)
        return copy

    barrier = pltpu.get_barrier_semaphore()
    peers = [{"row": rows[i], "col": cols[j]} for i, j in spots[1:]]
    peers += [{"front": near[1], "row": rows[i], "col": cols[j]} for i, j in spots]
    peers += [{"front": near[2]}, {"front": near[3]}]
    for where in peers:
        pl.semaphore_signal(barrier, inc=1, device_id=where, device_id_type=MESH)

    a_copies, om_copies = [], []

    def load_om(h):
        lanes = slice(HALF * h, HALF * h + HALF)
        copy = pltpu.make_async_copy(om_hbm.at[:, lanes], om_v.at[:, lanes], om_sem.at[h])
        copy.start()
        om_copies.append(copy)

    def load_a(s):
        i = len(a_copies)
        copy = pltpu.make_async_copy(
            a_hbm.at[:, pl.ds(pl.multiple_of(s * SUB, SUB), SUB), :], a_v.at[i], a_sem.at[i]
        )
        copy.start()
        a_copies.append(copy)

    load_om(0)
    load_a(cols[2])
    load_om(1)
    for s in (cols[1], cols[3], col):
        load_a(s)

    lane = lax.broadcasted_iota(jnp.int32, (8, BLK), 1)
    table = jnp.full((8, BLK), SRC, jnp.int32)
    for b in range(SRC):
        table = jnp.where(lane == map_ref[0, row * SRC + b], b, table)
    tab_v[0] = table
    for refs, (_, _, width) in zip(stage_refs, STAGES):
        for gat in refs[:2]:
            for k in range(4):
                gat[k, SRC] = jnp.zeros((8, width), jnp.float32)

    def multiply(i, h):
        product = jnp.dot(
            a_v[i].reshape(SRC * SUB, a_v.shape[-1]),
            om_v[:, HALF * h : HALF * h + HALF],
            preferred_element_type=jnp.float32,
        ).reshape(SRC, 4, 8, HALF)
        for q in range(4):
            part[i, h, q] = product[:, q]

    x_copy, c_copy, z_copy, f_copy, y_copy = {}, {}, {}, {}, {}

    def piece(i, h, t):
        q, lo, width = STAGES[t]
        return (i, h, q, slice(None), slice(None), slice(lo, lo + width))

    def send_x(t, d, step):
        i, h = ((0, d), (1 + d, 1 - d), (1 + d, d))[step]
        x_copy[t, d, step] = note(
            remote(
                part.at[piece(i, h, t)], stage_refs[t][2].at[d, step],
                x_ss.at[t, d, step], x_rs.at[t, d, step], col=cols[1] if d == 0 else cols[3],
            )
        )

    def pass_x(t):
        for d in (0, 1):
            x_copy[t, d, 0].wait_recv()
            at = piece(1 + d, d, t)
            part[at] = part[at] + stage_refs[t][2][d, 0]
            send_x(t, d, 2)

    def finish_x(t):
        for h in (0, 1):
            gat, got = stage_refs[t][h], stage_refs[t][2]
            x_copy[t, h, 2].wait_recv()
            x_copy[t, 1 - h, 1].wait_recv()
            gat[0, :SRC] = part[piece(3, h, t)] + (got[h, 2] + got[1 - h, 1])
            z_copy[t, h] = note(
                remote(gat.at[0, :SRC], gat.at[2, :SRC], z_ss.at[t, h], z_rs.at[t, h], front=near[2])
            )
            c_copy[t, h] = note(
                remote(gat.at[0, :SRC], gat.at[1, :SRC], c_ss.at[t, h], c_rs.at[t, h], front=near[1])
            )

    def forward_z(t):
        for h in (0, 1):
            gat = stage_refs[t][h]
            z_copy[t, h].wait_recv()
            f_copy[t, h] = note(
                remote(gat.at[2, :SRC], gat.at[3, :SRC], f_ss.at[t, h], f_rs.at[t, h], front=near[1])
            )

    def merge(t):
        for h in (0, 1):
            gat, _, ys, yr = stage_refs[t][h], *stage_refs[t][2:]
            c_copy[t, h].wait_recv()
            f_copy[t, h].wait_recv()
            for j in range(4 * OWN):
                at = sibling * (4 * OWN) + j
                ys[h, j] = (gat[0, tab_s[0, 0, at]] + gat[1, tab_s[1, 0, at]]) + (
                    gat[2, tab_s[2, 0, at]] + gat[3, tab_s[3, 0, at]]
                )
            for k in (1, 2, 3):
                y_copy[t, h, k] = note(
                    remote(
                        ys.at[h, pl.ds(OWN * rows[k], OWN)], yr.at[h, k - 1],
                        y_ss.at[t, h, k - 1], y_rs.at[t, h, k - 1], row=rows[k],
                    )
                )

    def finish_y(t):
        q, lo, width = STAGES[t]
        for h in (0, 1):
            _, ys, yr = stage_refs[t][2:]
            for k in (1, 2, 3):
                y_copy[t, h, k].wait_recv()
            all_v[:, col, 8 * q : 8 * q + 8, HALF * h + lo : HALF * h + lo + width] = (
                ys[h, pl.ds(OWN * row, OWN)] + yr[h, 0]
            ) + (yr[h, 1] + yr[h, 2])

    om_copies[0].wait()
    a_copies[0].wait()
    multiply(0, 0)
    pl.semaphore_wait(barrier, len(peers))
    send_x(0, 0, 0)
    send_x(1, 0, 0)
    om_copies[1].wait()
    multiply(0, 1)
    send_x(0, 1, 0)
    send_x(1, 1, 0)
    tab_copies = [
        remote(tab_v.at[0], tab_v.at[k], tab_ss.at[k - 1], tab_rs.at[k - 1], front=near[k]) for k in (1, 2, 3)
    ]
    a_copies[1].wait()
    multiply(1, 1)
    send_x(0, 0, 1)
    a_copies[2].wait()
    multiply(2, 0)
    send_x(0, 1, 1)
    multiply(1, 0)
    multiply(2, 1)
    a_copies[3].wait()
    count = len(STAGES)
    s_copy, w_copy = {}, {}

    def share_out(e, at):
        for d in (0, 1):
            block = all_v.at[:, col, at, :]
            s_copy[e, d] = note(
                remote(block, block, s_ss.at[e, d], s_rs.at[e, d], col=cols[1] if d == 0 else cols[3])
            )

    def pass_on(e, at):
        for d in (0, 1):
            s_copy[e, d].wait_recv()
            block = all_v.at[:, cols[3] if d == 0 else cols[1], at, HALF * d : HALF * d + HALF]
            w_copy[e, d] = note(
                remote(block, block, w_ss.at[e, d], w_rs.at[e, d], col=cols[1] if d == 0 else cols[3])
            )

    early, late = slice(0, 24), slice(24, 32)

    def add_gram(at, first):
        s = all_v[:, col, at, :].reshape(-1, 4 * BLK)
        base = 0
        for i in range(4):
            panel = dot(s[:, BLK * i : BLK * i + BLK], s[:, BLK * i :], ((0,), (0,)))
            for k in range(4 - i):
                block = panel[:, BLK * k : BLK * k + BLK]
                mine[base : base + BLK] = block if first else mine[base : base + BLK] + block
                base += BLK

    for tick in range(count + 4):
        if tick < count:
            pass_x(tick)
            for d in (0, 1):
                if tick + 2 < count:
                    send_x(tick + 2, d, 0)
                if tick + 1 < count:
                    send_x(tick + 1, d, 1)
        if tick == 0:
            multiply(3, 0)
            multiply(3, 1)
            for copy in tab_copies:
                copy.wait()
            tab_copy = pltpu.make_async_copy(tab_v, tab_s, tab_sem)
            tab_copy.start()
            tab_copy.wait()
        for action, lag in ((finish_x, 1), (forward_z, 2), (merge, 3), (finish_y, 4)):
            if 0 <= tick - lag < count:
                action(tick - lag)
        if tick - 4 == 2:
            share_out(0, early)
            add_gram(early, True)
    add_gram(late, False)

    def keep_rows(p):
        base, size = PARTS[p]
        half = size // 2
        return half, half // 16, lambda k: pl.ds(pl.multiple_of(base + half * k, 8), half)

    c1, yx, zz, bc = {}, {}, {}, {}
    for p in range(2):
        r1, ss, rs = part_refs[p][0], part_refs[p][5], part_refs[p][6]
        _, _, keep = keep_rows(p)
        c1[p] = note(remote(mine.at[keep(1 - core)], r1, ss, rs, front=near[1]))
    for p in range(2):
        r1, a1, r2 = part_refs[p][:3]
        ss, rs = part_refs[p][7:9]
        _, size, keep = keep_rows(p)
        c1[p].wait_recv()
        a1[...] = mine[keep(core)] + r1[...]
        for e, (i, j) in enumerate(spots[1:]):
            at = pl.ds(pl.multiple_of(size * (4 * rows[i] + cols[j]), 8), size)
            yx[p, e] = note(remote(a1.at[at], r2.at[e], ss.at[e], rs.at[e], row=rows[i], col=cols[j]))
    share_out(1, late)
    for p in range(2):
        _, a1, r2, a2, r3 = part_refs[p][:5]
        ss, rs = part_refs[p][9:11]
        _, size, _ = keep_rows(p)
        total = a1[pl.ds(pl.multiple_of(size * (4 * row + col), 8), size)]
        for e in range(15):
            yx[p, e].wait_recv()
            total = total + r2[e]
        a2[...] = total
        zz[p] = note(remote(a2, r3, ss, rs, front=near[2]))
    for p in range(2):
        a2, r3 = part_refs[p][3:5]
        ss, rs = part_refs[p][11:13]
        half, size, _ = keep_rows(p)
        base = PARTS[p][0]
        zz[p].wait_recv()
        at = pl.ds(pl.multiple_of(base + half * core + size * (4 * row + col), 8), size)
        gram[at] = a2[...] + r3[...]
        for e, (i, j) in enumerate(spots[1:]):
            bc[p, e] = note(
                remote(gram.at[at], gram.at[at], ss.at[e], rs.at[e], row=rows[i], col=cols[j])
            )
        if p == 1:
            for e, (i, j) in enumerate(spots):
                bc[p, 15 + e] = note(
                    remote(
                        gram.at[at], gram.at[at], ss.at[15 + e], rs.at[15 + e],
                        front=near[1], row=rows[i], col=cols[j],
                    )
                )
    for e in range(15):
        bc[0, e].wait_recv()
    _, _, keep = keep_rows(0)
    ends = part_refs[0][13]
    swap = note(remote(gram.at[keep(core)], gram.at[keep(core)], ends.at[0], ends.at[1], front=near[1]))
    pass_on(0, early)
    pass_on(1, late)
    swap.wait_recv()

    def unpack(p, panels):
        base = PARTS[p][0]
        for i in panels:
            for k in range(i, 4):
                a[i, :, BLK * k : BLK * k + BLK] = gram[base : base + BLK]
                base += BLK

    unpack(0, (0,))
    v[...] = jnp.zeros_like(v)
    for j in range(4):
        here = slice(BLK * j, BLK * j + BLK)

        def read(i):
            return a[j, 8 * i : 8 * i + 8, here]

        def write(i, block):
            v[j, 8 * i : 8 * i + 8, here] = block

        factor_inverse(read, write)
        if j == 0:
            for e in range(31):
                bc[1, e].wait_recv()
            unpack(1, (1, 2, 3))
        w = v[j, :, here]
        if j:
            v[j, :, : BLK * j] = dot(w, v[j, :, : BLK * j], ((1,), (0,)))
        if j < 3:
            u = dot(w, a[j, :, BLK * (j + 1) :], ((1,), (0,)))
            for i in range(j + 1, 4):
                part_u = u[:, BLK * (i - j - 1) : BLK * (i - j)]
                a[i, :, BLK * i :] = a[i, :, BLK * i :] - dot(part_u, u[:, BLK * (i - j - 1) :], ((0,), (0,)))
                v[i, :, : BLK * (j + 1)] = v[i, :, : BLK * (j + 1)] - dot(
                    part_u, v[j, :, : BLK * (j + 1)], ((0,), (0,))
                )
    for e in (0, 1):
        for d in (0, 1):
            w_copy[e, d].wait_recv()
    out_ref[...] = dot(v[col], all_v[...].reshape(OWN * BLK, 4 * BLK), ((1,), (1,)))
    for copy in pending:
        copy.wait_send()


def shards(child_blocks, sketch, block_map):
    f32, dma = jnp.float32, pltpu.SemaphoreType.DMA
    depth, width = sketch.shape
    count = len(STAGES)
    scratch = [
        pltpu.VMEM((4, SRC, SUB, depth), jnp.bfloat16),
        pltpu.VMEM((depth, width), jnp.bfloat16),
        pltpu.VMEM((4, 2, 4, SRC, 8, HALF), f32),
        pltpu.VMEM((4, 8, BLK), jnp.int32),
        pltpu.SMEM((4, 8, BLK), jnp.int32),
        pltpu.VMEM((OWN, 4, SUB, width), f32),
        pltpu.VMEM((10 * BLK, BLK), f32),
        pltpu.VMEM((10 * BLK, BLK), f32),
        pltpu.VMEM((4, BLK, width), f32),
        pltpu.VMEM((4, BLK, width), f32),
        dma((4,)), dma((2,)), dma, dma((3,)), dma((3,)),
        dma((count, 2, 3)), dma((count, 2, 3)),
    ]
    scratch += [dma((count, 2))] * 6 + [dma((count, 2, 3))] * 2 + [dma((2, 2))] * 4
    for _, _, w in STAGES:
        scratch += [
            pltpu.VMEM((4, SRC + 1, 8, w), f32),
            pltpu.VMEM((4, SRC + 1, 8, w), f32),
            pltpu.VMEM((2, 3, SRC, 8, w), f32),
            pltpu.VMEM((2, 4 * OWN, 8, w), f32),
            pltpu.VMEM((2, 3, OWN, 8, w), f32),
        ]
    for p, (_, size) in enumerate(PARTS):
        small = size // 32
        scratch += [
            pltpu.VMEM((size // 2, BLK), f32),
            pltpu.VMEM((size // 2, BLK), f32),
            pltpu.VMEM((15, small, BLK), f32),
            pltpu.VMEM((small, BLK), f32),
            pltpu.VMEM((small, BLK), f32),
            dma, dma, dma((15,)), dma((15,)), dma, dma, dma((31,)), dma((31,)), dma((2,)),
        ]
    return pl.pallas_call(
        kernel,
        out_shape=jax.ShapeDtypeStruct((BLK, OWN * BLK), f32),
        in_specs=[
            pl.BlockSpec(memory_space=pl.ANY),
            pl.BlockSpec(memory_space=pl.ANY),
            pl.BlockSpec(memory_space=pltpu.SMEM),
        ],
        out_specs=pl.BlockSpec(memory_space=pltpu.VMEM),
        scratch_shapes=scratch,
        compiler_params=pltpu.CompilerParams(collective_id=0, has_side_effects=True, vmem_limit_bytes=67043328),
        name="sketch_basis",
    )(child_blocks.reshape(SRC, BLK, depth), sketch, block_map)


def solution(mesh):
    placed = (P(("front", "row"), "col"), P("col", None), P("front", None))
    return jax.shard_map(
        shards, mesh=mesh, in_specs=placed, out_specs=P("col", ("front", "row")), check_vma=False
    )
```

```python
import jax
import jax.numpy as jnp
from jax import lax
from jax.experimental import pallas as pl
from jax.experimental.pallas import tpu as pltpu
from jax.sharding import PartitionSpec as P

MESH = pl.DeviceIdType.MESH
HIGHEST = lax.Precision.HIGHEST
BLK = 128
SUB = 32
SRC = 16
OWN = 6
HALF = 256
STAGES = [(0, 0, 256), (1, 0, 256), (2, 0, 128), (2, 128, 128), (3, 0, 128), (3, 128, 128)]
ORDER = "p0 m p1 x0 p2 x1 f0 e0 p3 x2 p4 f1 x3 e1 y0 f2 p5 e2 x4 f3 e3 x5 y1 f4 y2 e4 f5 y3 s e5 g y4 y5".split()
PARTS = ((0, 4 * BLK), (4 * BLK, 6 * BLK))


def remote(src, dst, send, recv, **where):
    copy = pltpu.make_async_remote_copy(
        src_ref=src, dst_ref=dst, send_sem=send, recv_sem=recv, device_id=where, device_id_type=MESH
    )
    copy.start()
    return copy


def settle(sem, like):
    pltpu.make_async_copy(like, like, sem).wait()


def around(axis):
    here = lax.axis_index(axis)
    return here, [lax.rem(here + step, 4) for step in range(4)]


def flip(front, bits):
    low = lax.rem(front, 4)
    core, half = lax.rem(low, 2), low // 2
    if bits & 1:
        core = 1 - core
    if bits & 2:
        half = 1 - half
    return front - low + 2 * half + core


def dot(x, y, dims):
    return lax.dot_general(x, y, (dims, ((), ())), precision=HIGHEST, preferred_element_type=jnp.float32)


def factor_inverse(read, write):
    sub = lax.broadcasted_iota(jnp.int32, (8, BLK), 0)
    lane = lax.broadcasted_iota(jnp.int32, (8, BLK), 1)
    count = BLK // 8
    upper = [read(i) for i in range(count)]
    inverse = [jnp.where(lane == sub + 8 * i, 1.0, 0.0).astype(jnp.float32) for i in range(count)]

    def spread(block, k):
        return jnp.broadcast_to(block[k : k + 1, :], (8, BLK))

    for j in range(count):
        below = range(j, count)
        column = {
            i: [jnp.broadcast_to(upper[i][:, 8 * j + k : 8 * j + k + 1], (8, BLK)) for k in range(8)]
            for i in below
        }
        lower = {i: [] for i in below}
        rest, solved = upper[j], inverse[j]
        u_rows, w_rows = [], []
        for k in range(8):
            scale = lax.rsqrt(spread(column[j][k], k))
            for i in below:
                lower[i].append(column[i][k] * scale)
            u_row, w_row = spread(rest, k) * scale, spread(solved, k) * scale
            u_rows.append(u_row)
            w_rows.append(w_row)
            under = jnp.where(sub > k, lower[j][k], 0.0)
            solved = jnp.where(sub == k, w_row, solved - under * w_row)
            rest = rest - under * u_row
            for later in range(k + 1, 8):
                factor = spread(lower[j][k], later)
                for i in below:
                    column[i][later] = column[i][later] - lower[i][k] * factor
        write(j, solved)
        for i in range(j + 1, count):
            for k in range(8):
                upper[i] = upper[i] - lower[i][k] * u_rows[k]
                inverse[i] = inverse[i] - lower[i][k] * w_rows[k]


def kernel(a_hbm, om_hbm, map_ref, out_ref, *scratch):
    left = iter(scratch)

    def take(count):
        return [next(left) for _ in range(count)]

    a_v, om_v, part, tab_v, tab_s, all_v, mine, gram, a, v = take(10)
    a_sem, om_sem, tab_sem, tab_ss, tab_rs = take(5)
    x_ss, m_rs, x_rs, g_ss, z_rs, g_rs, y_ss, y_rs, s_ss, s_rs, w_ss, w_rs = take(12)
    stage_refs = [take(5) for _ in STAGES]
    part_refs = [take(15) for _ in PARTS]

    front = lax.axis_index("front")
    sibling, core = lax.rem(front, 4), lax.rem(front, 2)
    row, rows = around("row")
    col, cols = around("col")
    near = [flip(front, bits) for bits in range(4)]
    spots = [(i, j) for i in range(4) for j in range(4)]

    barrier = pltpu.get_barrier_semaphore()
    peers = [{"row": rows[i], "col": cols[j]} for i, j in spots[1:]]
    peers += [{"front": near[1], "row": rows[i], "col": cols[j]} for i, j in spots]
    peers += [{"front": near[2]}, {"front": near[3]}]
    for where in peers:
        pl.semaphore_signal(barrier, inc=1, device_id=where, device_id_type=MESH)

    a_copies, om_copies = [], []

    def load_om(h):
        lanes = slice(HALF * h, HALF * h + HALF)
        copy = pltpu.make_async_copy(om_hbm.at[:, lanes], om_v.at[:, lanes], om_sem.at[h])
        copy.start()
        om_copies.append(copy)

    def load_a(s):
        i = len(a_copies)
        copy = pltpu.make_async_copy(
            a_hbm.at[:, pl.ds(pl.multiple_of(s * SUB, SUB), SUB), :], a_v.at[i], a_sem.at[i]
        )
        copy.start()
        a_copies.append(copy)

    load_om(0)
    load_a(cols[2])

    lane = lax.broadcasted_iota(jnp.int32, (8, BLK), 1)
    table = jnp.full((8, BLK), SRC, jnp.int32)
    for b in range(SRC):
        table = jnp.where(lane == map_ref[0, row * SRC + b], b, table)
    tab_v[0] = table
    for refs, (_, _, width) in zip(stage_refs, STAGES):
        for gat in refs[:2]:
            for k in range(4):
                gat[k, SRC] = jnp.zeros((8, width), jnp.float32)

    def multiply(i, h):
        product = jnp.dot(
            a_v[i].reshape(SRC * SUB, a_v.shape[-1]),
            om_v[:, HALF * h : HALF * h + HALF],
            preferred_element_type=jnp.float32,
        ).reshape(SRC, 4, 8, HALF)
        for q in range(4):
            part[i, h, q] = product[:, q]

    def piece(i, h, t):
        q, lo, width = STAGES[t]
        return (i, h, q, slice(None), slice(None), slice(lo, lo + width))

    def send_x(t, d, step):
        i, h = ((0, d), (1 + d, 1 - d), (1 + d, d))[step]
        remote(
            part.at[piece(i, h, t)], stage_refs[t][2].at[step, d],
            x_ss.at[t], (x_rs if step else m_rs).at[t], col=cols[1] if d == 0 else cols[3],
        )

    def pass_x(t):
        got = stage_refs[t][2]
        settle(m_rs.at[t], got.at[0])
        for d in (0, 1):
            at = piece(1 + d, d, t)
            part[at] = part[at] + got[0, d]
            send_x(t, d, 2)
        for step, after in ((1, t + 1), (0, t + 2)):
            if after < len(STAGES):
                for d in (0, 1):
                    send_x(after, d, step)

    def finish_x(t):
        got = stage_refs[t][2]
        settle(x_rs.at[t], got.at[1:3])
        for h in (0, 1):
            gat = stage_refs[t][h]
            gat[0, :SRC] = part[piece(3, h, t)] + (got[2, h] + got[1, 1 - h])
            remote(gat.at[0, :SRC], gat.at[2, :SRC], g_ss.at[t], z_rs.at[t], front=near[2])
            remote(gat.at[0, :SRC], gat.at[1, :SRC], g_ss.at[t], g_rs.at[t], front=near[1])

    def forward_z(t):
        settle(z_rs.at[t], stage_refs[t][2].at[0])
        for h in (0, 1):
            gat = stage_refs[t][h]
            remote(gat.at[2, :SRC], gat.at[3, :SRC], g_ss.at[t], g_rs.at[t], front=near[1])

    def merge(t):
        settle(g_rs.at[t], stage_refs[t][2].at[1:3])
        for h in (0, 1):
            gat, ys, yr = stage_refs[t][h], *stage_refs[t][3:]
            for j in range(4 * OWN):
                at = sibling * (4 * OWN) + j
                ys[h, j] = (gat[0, tab_s[0, 0, at]] + gat[1, tab_s[1, 0, at]]) + (
                    gat[2, tab_s[2, 0, at]] + gat[3, tab_s[3, 0, at]]
                )
            for k in (1, 2, 3):
                remote(
                    ys.at[h, pl.ds(OWN * rows[k], OWN)], yr.at[h, k - 1], y_ss.at[t], y_rs.at[t], row=rows[k]
                )

    def finish_y(t):
        q, lo, width = STAGES[t]
        ys, yr = stage_refs[t][3:]
        settle(y_rs.at[t], yr)
        for h in (0, 1):
            all_v[:, col, 8 * q : 8 * q + 8, HALF * h + lo : HALF * h + lo + width] = (
                ys[h, pl.ds(OWN * row, OWN)] + yr[h, 0]
            ) + (yr[h, 1] + yr[h, 2])

    om_copies[0].wait()
    a_copies[0].wait()
    load_om(1)
    for s in (cols[1], cols[3], col):
        load_a(s)
    multiply(0, 0)
    pl.semaphore_wait(barrier, len(peers))
    send_x(0, 0, 0)
    send_x(1, 0, 0)
    om_copies[1].wait()
    multiply(0, 1)
    send_x(0, 1, 0)
    send_x(1, 1, 0)
    for k in (1, 2, 3):
        remote(tab_v.at[0], tab_v.at[k], tab_ss, tab_rs, front=near[k])
    a_copies[1].wait()
    multiply(1, 1)
    send_x(0, 0, 1)
    a_copies[2].wait()
    multiply(2, 0)
    send_x(0, 1, 1)
    multiply(1, 0)
    multiply(2, 1)
    a_copies[3].wait()

    def share_out(e, at):
        for d in (0, 1):
            block = all_v.at[:, col, at, :]
            remote(block, block, s_ss.at[e], s_rs.at[e], col=cols[1] if d == 0 else cols[3])

    def pass_on(e, at):
        settle(s_rs.at[e], all_v.at[:, 0:2, at, :])
        for d in (0, 1):
            block = all_v.at[:, cols[3] if d == 0 else cols[1], at, HALF * d : HALF * d + HALF]
            remote(block, block, w_ss.at[e], w_rs.at[e], col=cols[1] if d == 0 else cols[3])

    early, late = slice(0, 24), slice(24, 32)

    def add_gram(at, first):
        s = all_v[:, col, at, :].reshape(-1, 4 * BLK)
        base = 0
        for i in range(4):
            panel = dot(s[:, BLK * i : BLK * i + BLK], s[:, BLK * i :], ((0,), (0,)))
            for k in range(4 - i):
                block = panel[:, BLK * k : BLK * k + BLK]
                mine[base : base + BLK] = block if first else mine[base : base + BLK] + block
                base += BLK

    def own_rows():
        multiply(3, 0)
        multiply(3, 1)
        settle(tab_rs, tab_v.at[1:4])
        tab_copy = pltpu.make_async_copy(tab_v, tab_s, tab_sem)
        tab_copy.start()
        tab_copy.wait()

    work = {"p": pass_x, "x": finish_x, "f": forward_z, "e": merge, "y": finish_y}
    other = {"m": own_rows, "s": lambda: share_out(0, early), "g": lambda: add_gram(early, True)}
    for item in ORDER:
        if item in other:
            other[item]()
        else:
            work[item[0]](int(item[1:]))
    add_gram(late, False)

    def keep_rows(p):
        base, size = PARTS[p]
        half = size // 2
        return half, half // 16, lambda k: pl.ds(pl.multiple_of(base + half * k, 8), half)

    for p in range(2):
        r1, ss, rs = part_refs[p][0], *part_refs[p][5:7]
        _, _, keep = keep_rows(p)
        remote(mine.at[keep(1 - core)], r1, ss, rs, front=near[1])
    for p in range(2):
        r1, a1, r2 = part_refs[p][:3]
        ss, rs = part_refs[p][7:9]
        _, size, keep = keep_rows(p)
        settle(part_refs[p][6], r1)
        a1[...] = mine[keep(core)] + r1[...]
        for e, (i, j) in enumerate(spots[1:]):
            at = pl.ds(pl.multiple_of(size * (4 * rows[i] + cols[j]), 8), size)
            remote(a1.at[at], r2.at[e], ss, rs, row=rows[i], col=cols[j])
    for p in range(2):
        _, a1, r2, a2, r3 = part_refs[p][:5]
        ss, rs = part_refs[p][9:11]
        _, size, _ = keep_rows(p)
        settle(part_refs[p][8], r2)
        total = a1[pl.ds(pl.multiple_of(size * (4 * row + col), 8), size)]
        for e in range(15):
            total = total + r2[e]
        a2[...] = total
        remote(a2, r3, ss, rs, front=near[2])
    for p in range(2):
        a2, r3 = part_refs[p][3:5]
        ss, rs = part_refs[p][11:13]
        half, size, _ = keep_rows(p)
        base = PARTS[p][0]
        settle(part_refs[p][10], r3)
        at = pl.ds(pl.multiple_of(base + half * core + size * (4 * row + col), 8), size)
        gram[at] = a2[...] + r3[...]
        for i, j in spots[1:]:
            remote(gram.at[at], gram.at[at], ss, rs, row=rows[i], col=cols[j])
        if p == 1:
            for i, j in spots:
                remote(gram.at[at], gram.at[at], ss, rs, front=near[1], row=rows[i], col=cols[j])
    share_out(1, late)
    settle(part_refs[0][12], part_refs[0][2])
    _, _, keep = keep_rows(0)
    swap_ss, swap_rs = part_refs[0][13:]
    remote(gram.at[keep(core)], gram.at[keep(core)], swap_ss, swap_rs, front=near[1])
    pass_on(0, early)
    settle(swap_rs, part_refs[0][0])
    everywhere = mine.at[: 31 * PARTS[1][1] // 32]

    def unpack(p, panels):
        base = PARTS[p][0]
        for i in panels:
            for k in range(i, 4):
                a[i, :, BLK * k : BLK * k + BLK] = gram[base : base + BLK]
                base += BLK

    unpack(0, (0,))
    v[...] = jnp.zeros_like(v)
    for j in range(4):
        here = slice(BLK * j, BLK * j + BLK)

        def read(i):
            return a[j, 8 * i : 8 * i + 8, here]

        def write(i, block):
            v[j, 8 * i : 8 * i + 8, here] = block

        factor_inverse(read, write)
        if j == 0:
            pass_on(1, late)
            settle(part_refs[1][12], everywhere)
            unpack(1, (1, 2, 3))
        w = v[j, :, here]
        if j:
            v[j, :, : BLK * j] = dot(w, v[j, :, : BLK * j], ((1,), (0,)))
        if j < 3:
            u = dot(w, a[j, :, BLK * (j + 1) :], ((1,), (0,)))
            for i in range(j + 1, 4):
                part_u = u[:, BLK * (i - j - 1) : BLK * (i - j)]
                a[i, :, BLK * i :] = a[i, :, BLK * i :] - dot(part_u, u[:, BLK * (i - j - 1) :], ((0,), (0,)))
                v[i, :, : BLK * (j + 1)] = v[i, :, : BLK * (j + 1)] - dot(
                    part_u, v[j, :, : BLK * (j + 1)], ((0,), (0,))
                )
    for e, at in enumerate((early, late)):
        settle(w_rs.at[e], all_v.at[:, 0, at, :])
    out_ref[...] = dot(v[col], all_v[...].reshape(OWN * BLK, 4 * BLK), ((1,), (1,)))
    settle(tab_ss, tab_v.at[1:4])
    for t, refs in enumerate(stage_refs):
        settle(x_ss.at[t], refs[2])
        settle(g_ss.at[t], refs[2])
        settle(y_ss.at[t], refs[4])
    for e, at in enumerate((early, late)):
        settle(s_ss.at[e], all_v.at[:, 0:2, at, :])
        settle(w_ss.at[e], all_v.at[:, 0, at, :])
    for p in range(2):
        refs = part_refs[p]
        settle(refs[5], refs[0])
        settle(refs[7], refs[2])
        settle(refs[9], refs[3])
        settle(refs[11], everywhere if p else refs[2])
    settle(swap_ss, part_refs[0][0])


def shards(child_blocks, sketch, block_map):
    f32, dma = jnp.float32, pltpu.SemaphoreType.DMA
    depth, width = sketch.shape
    count = len(STAGES)
    scratch = [
        pltpu.VMEM((4, SRC, SUB, depth), jnp.bfloat16),
        pltpu.VMEM((depth, width), jnp.bfloat16),
        pltpu.VMEM((4, 2, 4, SRC, 8, HALF), f32),
        pltpu.VMEM((4, 8, BLK), jnp.int32),
        pltpu.SMEM((4, 8, BLK), jnp.int32),
        pltpu.VMEM((OWN, 4, SUB, width), f32),
        pltpu.VMEM((10 * BLK, BLK), f32),
        pltpu.VMEM((10 * BLK, BLK), f32),
        pltpu.VMEM((4, BLK, width), f32),
        pltpu.VMEM((4, BLK, width), f32),
        dma((4,)), dma((2,)), dma, dma, dma,
    ]
    scratch += [dma((count,))] * 8 + [dma((2,))] * 4
    for _, _, w in STAGES:
        scratch += [
            pltpu.VMEM((4, SRC + 1, 8, w), f32),
            pltpu.VMEM((4, SRC + 1, 8, w), f32),
            pltpu.VMEM((3, 2, SRC, 8, w), f32),
            pltpu.VMEM((2, 4 * OWN, 8, w), f32),
            pltpu.VMEM((2, 3, OWN, 8, w), f32),
        ]
    for p, (_, size) in enumerate(PARTS):
        small = size // 32
        scratch += [
            pltpu.VMEM((size // 2, BLK), f32),
            pltpu.VMEM((size // 2, BLK), f32),
            pltpu.VMEM((15, small, BLK), f32),
            pltpu.VMEM((small, BLK), f32),
            pltpu.VMEM((small, BLK), f32),
        ] + [dma] * 10
    return pl.pallas_call(
        kernel,
        out_shape=jax.ShapeDtypeStruct((BLK, OWN * BLK), f32),
        in_specs=[
            pl.BlockSpec(memory_space=pl.ANY),
            pl.BlockSpec(memory_space=pl.ANY),
            pl.BlockSpec(memory_space=pltpu.SMEM),
        ],
        out_specs=pl.BlockSpec(memory_space=pltpu.VMEM),
        scratch_shapes=scratch,
        compiler_params=pltpu.CompilerParams(collective_id=0, has_side_effects=True, vmem_limit_bytes=67043328),
        name="sketch_basis",
    )(child_blocks.reshape(SRC, BLK, depth), sketch, block_map)


def solution(mesh):
    placed = (P(("front", "row"), "col"), P("col", None), P("front", None))
    return jax.shard_map(
        shards, mesh=mesh, in_specs=placed, out_specs=P("col", ("front", "row")), check_vma=False
    )
```

```python
import jax
import jax.numpy as jnp
from jax import lax
from jax.experimental import pallas as pl
from jax.experimental.pallas import tpu as pltpu
from jax.sharding import PartitionSpec as P

MESH = pl.DeviceIdType.MESH
HIGHEST = lax.Precision.HIGHEST
BLK = 128
SUB = 32
SRC = 16
OWN = 6
HALF = 256
STAGES = [(0, 0, 256), (1, 0, 256), (2, 0, 128), (2, 128, 128), (3, 0, 128), (3, 128, 128)]
ORDER = "p0 m p1 x0 p2 x1 f0 e0 p3 x2 p4 f1 x3 e1 y0 f2 p5 e2 x4 f3 e3 x5 y1 f4 y2 e4 f5 y3 s e5 g y4 y5".split()
PARTS = ((0, 4 * BLK), (4 * BLK, 6 * BLK))


def remote(src, dst, send, recv, **where):
    copy = pltpu.make_async_remote_copy(
        src_ref=src, dst_ref=dst, send_sem=send, recv_sem=recv, device_id=where, device_id_type=MESH
    )
    copy.start()
    return copy


def settle(sem, like):
    pltpu.make_async_copy(like, like, sem).wait()


def around(axis):
    here = lax.axis_index(axis)
    return here, [lax.rem(here + step, 4) for step in range(4)]


def flip(front, bits):
    low = lax.rem(front, 4)
    core, half = lax.rem(low, 2), low // 2
    if bits & 1:
        core = 1 - core
    if bits & 2:
        half = 1 - half
    return front - low + 2 * half + core


def dot(x, y, dims):
    return lax.dot_general(x, y, (dims, ((), ())), precision=HIGHEST, preferred_element_type=jnp.float32)


def factor_inverse(read, write):
    sub = lax.broadcasted_iota(jnp.int32, (8, BLK), 0)
    lane = lax.broadcasted_iota(jnp.int32, (8, BLK), 1)
    count = BLK // 8
    upper = [read(i) for i in range(count)]
    inverse = [jnp.where(lane == sub + 8 * i, 1.0, 0.0).astype(jnp.float32) for i in range(count)]

    def spread(block, k):
        return jnp.broadcast_to(block[k : k + 1, :], (8, BLK))

    def columns(block, j):
        return [jnp.broadcast_to(block[:, 8 * j + k : 8 * j + k + 1], (8, BLK)) for k in range(8)]

    ahead = columns(upper[0], 0)
    for j in range(count):
        below = range(j, count)
        column = {i: columns(upper[i], j) for i in range(j + 1, count)}
        column[j] = ahead
        ahead = columns(upper[j + 1], j + 1) if j + 1 < count else []
        lower = {i: [] for i in below}
        rest, solved = upper[j], inverse[j]
        u_rows, w_rows = [], []
        for k in range(8):
            scale = lax.rsqrt(spread(column[j][k], k))
            for i in below:
                lower[i].append(column[i][k] * scale)
            u_row, w_row = spread(rest, k) * scale, spread(solved, k) * scale
            u_rows.append(u_row)
            w_rows.append(w_row)
            under = jnp.where(sub > k, lower[j][k], 0.0)
            solved = jnp.where(sub == k, w_row, solved - under * w_row)
            rest = rest - under * u_row
            for later in range(k + 1, 8):
                factor = spread(lower[j][k], later)
                for i in below:
                    column[i][later] = column[i][later] - lower[i][k] * factor
            for c in range(len(ahead)):
                ahead[c] = ahead[c] - lower[j + 1][k] * spread(lower[j + 1][k], c)
        write(j, solved)
        for i in range(j + 1, count):
            for k in range(8):
                upper[i] = upper[i] - lower[i][k] * u_rows[k]
                inverse[i] = inverse[i] - lower[i][k] * w_rows[k]


def kernel(a_hbm, om_hbm, map_ref, out_ref, *scratch):
    left = iter(scratch)

    def take(count):
        return [next(left) for _ in range(count)]

    a_v, om_v, part, tab_v, tab_s, all_v, mine, gram, a, v = take(10)
    a_sem, om_sem, tab_sem, tab_ss, tab_rs = take(5)
    x_ss, m_rs, x_rs, g_ss, z_rs, g_rs, y_ss, y_rs, s_ss, s_rs, w_ss, w_rs = take(12)
    stage_refs = [take(5) for _ in STAGES]
    part_refs = [take(15) for _ in PARTS]

    front = lax.axis_index("front")
    sibling, core = lax.rem(front, 4), lax.rem(front, 2)
    row, rows = around("row")
    col, cols = around("col")
    near = [flip(front, bits) for bits in range(4)]
    spots = [(i, j) for i in range(4) for j in range(4)]

    barrier = pltpu.get_barrier_semaphore()
    peers = [{"row": rows[i], "col": cols[j]} for i, j in spots[1:]]
    peers += [{"front": near[1], "row": rows[i], "col": cols[j]} for i, j in spots]
    peers += [{"front": near[2]}, {"front": near[3]}]
    for where in peers:
        pl.semaphore_signal(barrier, inc=1, device_id=where, device_id_type=MESH)

    a_copies, om_copies = [], []

    def load_om(h):
        lanes = slice(HALF * h, HALF * h + HALF)
        copy = pltpu.make_async_copy(om_hbm.at[:, lanes], om_v.at[:, lanes], om_sem.at[h])
        copy.start()
        om_copies.append(copy)

    def load_a(s):
        i = len(a_copies)
        copy = pltpu.make_async_copy(
            a_hbm.at[:, pl.ds(pl.multiple_of(s * SUB, SUB), SUB), :], a_v.at[i], a_sem.at[i]
        )
        copy.start()
        a_copies.append(copy)

    load_om(0)
    load_a(cols[2])
    load_om(1)
    for s in (cols[1], cols[3], col):
        load_a(s)

    lane = lax.broadcasted_iota(jnp.int32, (8, BLK), 1)
    table = jnp.full((8, BLK), SRC, jnp.int32)
    for b in range(SRC):
        table = jnp.where(lane == map_ref[0, row * SRC + b], b, table)
    tab_v[0] = table
    for refs, (_, _, width) in zip(stage_refs, STAGES):
        for gat in refs[:2]:
            for k in range(4):
                gat[k, SRC] = jnp.zeros((8, width), jnp.float32)

    def multiply(i, h):
        product = jnp.dot(
            a_v[i].reshape(SRC * SUB, a_v.shape[-1]),
            om_v[:, HALF * h : HALF * h + HALF],
            preferred_element_type=jnp.float32,
        ).reshape(SRC, 4, 8, HALF)
        for q in range(4):
            part[i, h, q] = product[:, q]

    def piece(i, h, t):
        q, lo, width = STAGES[t]
        return (i, h, q, slice(None), slice(None), slice(lo, lo + width))

    def send_x(t, d, step):
        i, h = ((0, d), (1 + d, 1 - d), (1 + d, d))[step]
        remote(
            part.at[piece(i, h, t)], stage_refs[t][2].at[step, d],
            x_ss.at[t], (x_rs if step else m_rs).at[t], col=cols[1] if d == 0 else cols[3],
        )

    def pass_x(t):
        got = stage_refs[t][2]
        settle(m_rs.at[t], got.at[0])
        for d in (0, 1):
            at = piece(1 + d, d, t)
            part[at] = part[at] + got[0, d]
            send_x(t, d, 2)
        for step, after in ((1, t + 1), (0, t + 2)):
            if after < len(STAGES):
                for d in (0, 1):
                    send_x(after, d, step)

    def finish_x(t):
        got = stage_refs[t][2]
        settle(x_rs.at[t], got.at[1:3])
        for h in (0, 1):
            gat = stage_refs[t][h]
            gat[0, :SRC] = part[piece(3, h, t)] + (got[2, h] + got[1, 1 - h])
            remote(gat.at[0, :SRC], gat.at[2, :SRC], g_ss.at[t], z_rs.at[t], front=near[2])
            remote(gat.at[0, :SRC], gat.at[1, :SRC], g_ss.at[t], g_rs.at[t], front=near[1])

    def forward_z(t):
        settle(z_rs.at[t], stage_refs[t][2].at[0])
        for h in (0, 1):
            gat = stage_refs[t][h]
            remote(gat.at[2, :SRC], gat.at[3, :SRC], g_ss.at[t], g_rs.at[t], front=near[1])

    def merge(t):
        settle(g_rs.at[t], stage_refs[t][2].at[1:3])
        for h in (0, 1):
            gat, ys, yr = stage_refs[t][h], *stage_refs[t][3:]
            for j in range(4 * OWN):
                at = sibling * (4 * OWN) + j
                ys[h, j] = (gat[0, tab_s[0, 0, at]] + gat[1, tab_s[1, 0, at]]) + (
                    gat[2, tab_s[2, 0, at]] + gat[3, tab_s[3, 0, at]]
                )
            for k in (1, 2, 3):
                remote(
                    ys.at[h, pl.ds(OWN * rows[k], OWN)], yr.at[h, k - 1], y_ss.at[t], y_rs.at[t], row=rows[k]
                )

    def finish_y(t):
        q, lo, width = STAGES[t]
        ys, yr = stage_refs[t][3:]
        settle(y_rs.at[t], yr)
        for h in (0, 1):
            all_v[:, col, 8 * q : 8 * q + 8, HALF * h + lo : HALF * h + lo + width] = (
                ys[h, pl.ds(OWN * row, OWN)] + yr[h, 0]
            ) + (yr[h, 1] + yr[h, 2])

    om_copies[0].wait()
    a_copies[0].wait()
    multiply(0, 0)
    pl.semaphore_wait(barrier, len(peers))
    send_x(0, 0, 0)
    send_x(1, 0, 0)
    om_copies[1].wait()
    multiply(0, 1)
    send_x(0, 1, 0)
    send_x(1, 1, 0)
    for k in (1, 2, 3):
        remote(tab_v.at[0], tab_v.at[k], tab_ss, tab_rs, front=near[k])
    a_copies[1].wait()
    multiply(1, 1)
    send_x(0, 0, 1)
    a_copies[2].wait()
    multiply(2, 0)
    send_x(0, 1, 1)
    multiply(1, 0)
    multiply(2, 1)
    a_copies[3].wait()

    def share_out(e, at):
        for d in (0, 1):
            block = all_v.at[:, col, at, :]
            remote(block, block, s_ss.at[e], s_rs.at[e], col=cols[1] if d == 0 else cols[3])

    def pass_on(e, at):
        settle(s_rs.at[e], all_v.at[:, 0:2, at, :])
        for d in (0, 1):
            block = all_v.at[:, cols[3] if d == 0 else cols[1], at, HALF * d : HALF * d + HALF]
            remote(block, block, w_ss.at[e], w_rs.at[e], col=cols[1] if d == 0 else cols[3])

    early, late = slice(0, 24), slice(24, 32)

    def add_gram(at, first):
        s = all_v[:, col, at, :].reshape(-1, 4 * BLK)
        base = 0
        for i in range(4):
            panel = dot(s[:, BLK * i : BLK * i + BLK], s[:, BLK * i :], ((0,), (0,)))
            for k in range(4 - i):
                block = panel[:, BLK * k : BLK * k + BLK]
                mine[base : base + BLK] = block if first else mine[base : base + BLK] + block
                base += BLK

    def own_rows():
        multiply(3, 0)
        multiply(3, 1)
        settle(tab_rs, tab_v.at[1:4])
        tab_copy = pltpu.make_async_copy(tab_v, tab_s, tab_sem)
        tab_copy.start()
        tab_copy.wait()

    work = {"p": pass_x, "x": finish_x, "f": forward_z, "e": merge, "y": finish_y}
    other = {"m": own_rows, "s": lambda: share_out(0, early), "g": lambda: add_gram(early, True)}
    for item in ORDER:
        if item in other:
            other[item]()
        else:
            work[item[0]](int(item[1:]))
    add_gram(late, False)

    def keep_rows(p):
        base, size = PARTS[p]
        half = size // 2
        return half, half // 16, lambda k: pl.ds(pl.multiple_of(base + half * k, 8), half)

    for p in range(2):
        r1, ss, rs = part_refs[p][0], *part_refs[p][5:7]
        _, _, keep = keep_rows(p)
        remote(mine.at[keep(1 - core)], r1, ss, rs, front=near[1])
    for p in range(2):
        r1, a1, r2 = part_refs[p][:3]
        ss, rs = part_refs[p][7:9]
        _, size, keep = keep_rows(p)
        settle(part_refs[p][6], r1)
        a1[...] = mine[keep(core)] + r1[...]
        for e, (i, j) in enumerate(spots[1:]):
            at = pl.ds(pl.multiple_of(size * (4 * rows[i] + cols[j]), 8), size)
            remote(a1.at[at], r2.at[e], ss, rs, row=rows[i], col=cols[j])
    for p in range(2):
        _, a1, r2, a2, r3 = part_refs[p][:5]
        ss, rs = part_refs[p][9:11]
        _, size, _ = keep_rows(p)
        settle(part_refs[p][8], r2)
        total = a1[pl.ds(pl.multiple_of(size * (4 * row + col), 8), size)]
        for e in range(15):
            total = total + r2[e]
        a2[...] = total
        remote(a2, r3, ss, rs, front=near[2])
    for p in range(2):
        a2, r3 = part_refs[p][3:5]
        ss, rs = part_refs[p][11:13]
        half, size, _ = keep_rows(p)
        base = PARTS[p][0]
        settle(part_refs[p][10], r3)
        at = pl.ds(pl.multiple_of(base + half * core + size * (4 * row + col), 8), size)
        gram[at] = a2[...] + r3[...]
        for i, j in spots[1:]:
            remote(gram.at[at], gram.at[at], ss, rs, row=rows[i], col=cols[j])
        if p == 1:
            for i, j in spots:
                remote(gram.at[at], gram.at[at], ss, rs, front=near[1], row=rows[i], col=cols[j])
    share_out(1, late)
    settle(part_refs[0][12], part_refs[0][2])
    _, _, keep = keep_rows(0)
    swap_ss, swap_rs = part_refs[0][13:]
    remote(gram.at[keep(core)], gram.at[keep(core)], swap_ss, swap_rs, front=near[1])
    pass_on(0, early)
    settle(swap_rs, part_refs[0][0])
    everywhere = mine.at[: 31 * PARTS[1][1] // 32]

    def unpack(p, panels):
        base = PARTS[p][0]
        for i in panels:
            for k in range(i, 4):
                a[i, :, BLK * k : BLK * k + BLK] = gram[base : base + BLK]
                base += BLK

    unpack(0, (0,))
    v[...] = jnp.zeros_like(v)
    for j in range(4):
        here = slice(BLK * j, BLK * j + BLK)

        def read(i):
            return a[j, 8 * i : 8 * i + 8, here]

        def write(i, block):
            v[j, 8 * i : 8 * i + 8, here] = block

        factor_inverse(read, write)
        if j == 0:
            pass_on(1, late)
            settle(part_refs[1][12], everywhere)
            unpack(1, (1, 2, 3))
        w = v[j, :, here]
        if j:
            v[j, :, : BLK * j] = dot(w, v[j, :, : BLK * j], ((1,), (0,)))
        if j < 3:
            u = dot(w, a[j, :, BLK * (j + 1) :], ((1,), (0,)))
            for i in range(j + 1, 4):
                part_u = u[:, BLK * (i - j - 1) : BLK * (i - j)]
                a[i, :, BLK * i :] = a[i, :, BLK * i :] - dot(part_u, u[:, BLK * (i - j - 1) :], ((0,), (0,)))
                v[i, :, : BLK * (j + 1)] = v[i, :, : BLK * (j + 1)] - dot(
                    part_u, v[j, :, : BLK * (j + 1)], ((0,), (0,))
                )
    for e, at in enumerate((early, late)):
        settle(w_rs.at[e], all_v.at[:, 0, at, :])
    out_ref[...] = dot(v[col], all_v[...].reshape(OWN * BLK, 4 * BLK), ((1,), (1,)))
    settle(tab_ss, tab_v.at[1:4])
    for t, refs in enumerate(stage_refs):
        settle(x_ss.at[t], refs[2])
        settle(g_ss.at[t], refs[2])
        settle(y_ss.at[t], refs[4])
    for e, at in enumerate((early, late)):
        settle(s_ss.at[e], all_v.at[:, 0:2, at, :])
        settle(w_ss.at[e], all_v.at[:, 0, at, :])
    for p in range(2):
        refs = part_refs[p]
        settle(refs[5], refs[0])
        settle(refs[7], refs[2])
        settle(refs[9], refs[3])
        settle(refs[11], everywhere if p else refs[2])
    settle(swap_ss, part_refs[0][0])


def shards(child_blocks, sketch, block_map):
    f32, dma = jnp.float32, pltpu.SemaphoreType.DMA
    depth, width = sketch.shape
    count = len(STAGES)
    scratch = [
        pltpu.VMEM((4, SRC, SUB, depth), jnp.bfloat16),
        pltpu.VMEM((depth, width), jnp.bfloat16),
        pltpu.VMEM((4, 2, 4, SRC, 8, HALF), f32),
        pltpu.VMEM((4, 8, BLK), jnp.int32),
        pltpu.SMEM((4, 8, BLK), jnp.int32),
        pltpu.VMEM((OWN, 4, SUB, width), f32),
        pltpu.VMEM((10 * BLK, BLK), f32),
        pltpu.VMEM((10 * BLK, BLK), f32),
        pltpu.VMEM((4, BLK, width), f32),
        pltpu.VMEM((4, BLK, width), f32),
        dma((4,)), dma((2,)), dma, dma, dma,
    ]
    scratch += [dma((count,))] * 8 + [dma((2,))] * 4
    for _, _, w in STAGES:
        scratch += [
            pltpu.VMEM((4, SRC + 1, 8, w), f32),
            pltpu.VMEM((4, SRC + 1, 8, w), f32),
            pltpu.VMEM((3, 2, SRC, 8, w), f32),
            pltpu.VMEM((2, 4 * OWN, 8, w), f32),
            pltpu.VMEM((2, 3, OWN, 8, w), f32),
        ]
    for p, (_, size) in enumerate(PARTS):
        small = size // 32
        scratch += [
            pltpu.VMEM((size // 2, BLK), f32),
            pltpu.VMEM((size // 2, BLK), f32),
            pltpu.VMEM((15, small, BLK), f32),
            pltpu.VMEM((small, BLK), f32),
            pltpu.VMEM((small, BLK), f32),
        ] + [dma] * 10
    return pl.pallas_call(
        kernel,
        out_shape=jax.ShapeDtypeStruct((BLK, OWN * BLK), f32),
        in_specs=[
            pl.BlockSpec(memory_space=pl.ANY),
            pl.BlockSpec(memory_space=pl.ANY),
            pl.BlockSpec(memory_space=pltpu.SMEM),
        ],
        out_specs=pl.BlockSpec(memory_space=pltpu.VMEM),
        scratch_shapes=scratch,
        compiler_params=pltpu.CompilerParams(collective_id=0, has_side_effects=True, vmem_limit_bytes=67043328),
        name="sketch_basis",
    )(child_blocks.reshape(SRC, BLK, depth), sketch, block_map)


def solution(mesh):
    placed = (P(("front", "row"), "col"), P("col", None), P("front", None))
    return jax.shard_map(
        shards, mesh=mesh, in_specs=placed, out_specs=P("col", ("front", "row")), check_vma=False
    )
```
